32 devices in a mesh: tp: 4 (over z), fsdp: 8 (over y, x, core).
Axes of the slice: x: 2, y: 2, z: 4, core: 2. Of those that a mesh axis runs over, the one named last changes fastest.
Arguments:
- hidden: bfloat16 [32, 256, 3072], P('fsdp')
- positions: int32 [32, 256], P('fsdp')
- grad_layer: bfloat16 [32, 256, 3072], P('fsdp')
- ln_weight: bfloat16 [3072], P('fsdp')
- w_query: bfloat16 [3072, 3072], P('fsdp', 'tp')
- w_key: bfloat16 [3072, 1024], P('fsdp', 'tp')
- w_value: bfloat16 [3072, 1024], P('fsdp', 'tp')
- w_out: bfloat16 [3072, 3072], P('tp', 'fsdp')
- w_gate: bfloat16 [3072, 8192], P('fsdp', 'tp')
- w_up: bfloat16 [3072, 8192], P('fsdp', 'tp')
- w_down: bfloat16 [8192, 3072], P('tp', 'fsdp')
- q_norm: bfloat16 [24, 128], P('tp', 'fsdp')
- k_norm: bfloat16 [8, 128], P('tp', 'fsdp')
Outputs:
- output 1: bfloat16 [32, 256, 3072], P('fsdp')
- output 2: bfloat16 [32, 256, 3072], P('fsdp')
- output 3: float32 [3072], P('fsdp')
- output 4: bfloat16 [3072, 3072], P('fsdp', 'tp')
- output 5: bfloat16 [3072, 1024], P('fsdp', 'tp')
- output 6: bfloat16 [3072, 1024], P('fsdp', 'tp')
- output 7: bfloat16 [3072, 3072], P('tp', 'fsdp')
- output 8: bfloat16 [3072, 8192], P('fsdp', 'tp')
- output 9: bfloat16 [3072, 8192], P('fsdp', 'tp')
- output 10: bfloat16 [8192, 3072], P('tp', 'fsdp')
- output 11: float32 [24, 128], P('tp', 'fsdp')
- output 12: float32 [8, 128], P('tp', 'fsdp')
All inputs are finite; a program needn't handle non-finite values.
Results may differ from the reference program's by a relative error of at most 0.02.
Values are sent between devices in bfloat16 or wider.
A program may use at most 1 GiB of HBM per device.

```python
import jax
import jax.numpy as jnp
from jax import lax

MODEL_DIM = 3072
NUM_HEADS = 24
KV_HEADS = 8
HEAD_DIM = 128
FFN_DIM = 8192
BATCH_TOTAL = 32
SEQ_LEN = 256
LN_EPS = 1e-5
ROPE_BASE = 10000.0


def setup_inputs(seed: int = 0) -> dict:
    keys = jax.random.split(jax.random.key(seed), 14)
    q_width = NUM_HEADS * HEAD_DIM
    kv_width = KV_HEADS * HEAD_DIM
    act_shape = (BATCH_TOTAL, SEQ_LEN, MODEL_DIM)
    hidden = jax.random.normal(keys[0], act_shape, jnp.float32).astype(jnp.bfloat16)
    grad_layer = jax.random.normal(keys[1], act_shape, jnp.float32).astype(jnp.bfloat16)
    start = jax.random.randint(keys[2], (BATCH_TOTAL, 1), 0, 1024)
    gaps = jax.random.randint(keys[3], (BATCH_TOTAL, SEQ_LEN), 1, 4)
    positions = (start + jnp.cumsum(gaps, axis=1) - gaps[:, :1]).astype(jnp.int32)

    def draw_weight(rng_key, fan_in, fan_out):
        return (jax.random.normal(rng_key, (fan_in, fan_out), jnp.float32) * fan_in ** -0.5).astype(jnp.bfloat16)

    def draw_gain(rng_key, shape, low, high):
        return jax.random.uniform(rng_key, shape, jnp.float32, low, high).astype(jnp.bfloat16)

    return {
        'hidden': hidden,
        'positions': positions,
        'grad_layer': grad_layer,
        'ln_weight': draw_gain(keys[4], (MODEL_DIM,), 0.5, 1.5),
        'w_query': draw_weight(keys[5], MODEL_DIM, q_width),
        'w_key': draw_weight(keys[6], MODEL_DIM, kv_width),
        'w_value': draw_weight(keys[7], MODEL_DIM, kv_width),
        'w_out': draw_weight(keys[8], q_width, MODEL_DIM),
        'w_gate': draw_weight(keys[9], MODEL_DIM, FFN_DIM),
        'w_up': draw_weight(keys[10], MODEL_DIM, FFN_DIM),
        'w_down': draw_weight(keys[11], FFN_DIM, MODEL_DIM),
        'q_norm': draw_gain(keys[12], (NUM_HEADS, HEAD_DIM), 0.75, 2.25),
        'k_norm': draw_gain(keys[13], (KV_HEADS, HEAD_DIM), 0.75, 2.25),
    }


def to_bf(tensor):
    return tensor.astype(jnp.bfloat16).astype(jnp.float32)


def layer_norm(tensor, weight):
    centered = tensor - jnp.mean(tensor, axis=-1, keepdims=True)
    variance = jnp.mean(centered * centered, axis=-1, keepdims=True)
    return centered * lax.rsqrt(variance + LN_EPS) * weight


def rotary(tensor, cosine, sine):
    pairs = tensor.reshape(tensor.shape[:-1] + (HEAD_DIM // 2, 2))
    first = pairs[..., 0]
    second = pairs[..., 1]
    turned = jnp.stack([first * cosine - second * sine, second * cosine + first * sine], axis=-1)
    return turned.reshape(tensor.shape)


def one_sequence(hid_seq, pos_seq, weights):
    ln_weight, w_query, w_key, w_value, w_out, w_gate, w_up, w_down, q_norm, k_norm = weights
    group = NUM_HEADS // KV_HEADS
    normed = to_bf(layer_norm(hid_seq, ln_weight))
    query = to_bf(jnp.dot(normed, w_query, preferred_element_type=jnp.float32))
    key_proj = to_bf(jnp.dot(normed, w_key, preferred_element_type=jnp.float32))
    value_proj = to_bf(jnp.dot(normed, w_value, preferred_element_type=jnp.float32))
    inv_freq = ROPE_BASE ** (-jnp.arange(0, HEAD_DIM, 2, dtype=jnp.float32) / HEAD_DIM)
    angles = pos_seq.astype(jnp.float32)[:, None, None] * inv_freq
    cosine = jnp.cos(angles)
    sine = jnp.sin(angles)
    q_rot = to_bf(rotary(layer_norm(query.reshape(SEQ_LEN, NUM_HEADS, HEAD_DIM), q_norm), cosine, sine))
    k_rot = to_bf(rotary(layer_norm(key_proj.reshape(SEQ_LEN, KV_HEADS, HEAD_DIM), k_norm), cosine, sine))
    value_heads = value_proj.reshape(SEQ_LEN, KV_HEADS, HEAD_DIM)
    q_rot = q_rot.reshape(SEQ_LEN, KV_HEADS, group, HEAD_DIM)
    scores = jnp.einsum('qkgd,skd->kgqs', q_rot, k_rot) * HEAD_DIM ** -0.5
    causal = jnp.arange(SEQ_LEN)[:, None] >= jnp.arange(SEQ_LEN)[None, :]
    attn_probs = to_bf(jax.nn.softmax(jnp.where(causal, scores, -1e30), axis=-1))
    attn_out = to_bf(jnp.einsum('kgqs,skd->qkgd', attn_probs, value_heads)).reshape(SEQ_LEN, NUM_HEADS * HEAD_DIM)
    attn_part = jnp.dot(attn_out, w_out, preferred_element_type=jnp.float32)
    gate = to_bf(jnp.dot(normed, w_gate, preferred_element_type=jnp.float32))
    up_proj = to_bf(jnp.dot(normed, w_up, preferred_element_type=jnp.float32))
    gated_act = to_bf(jax.nn.silu(gate) * up_proj)
    mlp_part = jnp.dot(gated_act, w_down, preferred_element_type=jnp.float32)
    return to_bf(hid_seq + attn_part + mlp_part)


def reference(hidden, positions, grad_layer, ln_weight, w_query, w_key, w_value, w_out, w_gate, w_up, w_down, q_norm, k_norm):
    weights_f32 = tuple(weight.astype(jnp.float32) for weight in (ln_weight, w_query, w_key, w_value, w_out, w_gate, w_up, w_down, q_norm, k_norm))

    def forward(hid_all, weights):
        def per_sequence(pair):
            return jax.checkpoint(one_sequence)(pair[0], pair[1], weights)
        return lax.map(per_sequence, (hid_all, positions))

    layer_out, pullback = jax.vjp(forward, hidden.astype(jnp.float32), weights_f32)
    grad_hidden, gradients = pullback(grad_layer.astype(jnp.float32))
    return (layer_out.astype(jnp.bfloat16), grad_hidden.astype(jnp.bfloat16), gradients[0],
            gradients[1].astype(jnp.bfloat16), gradients[2].astype(jnp.bfloat16), gradients[3].astype(jnp.bfloat16),
            gradients[4].astype(jnp.bfloat16), gradients[5].astype(jnp.bfloat16), gradients[6].astype(jnp.bfloat16),
            gradients[7].astype(jnp.bfloat16), gradients[8], gradients[9])
```

```python
import functools

import jax
import jax.numpy as jnp
from jax import lax
from jax.experimental import pallas as pl
from jax.experimental.pallas import tpu as pltpu
from jax.sharding import PartitionSpec as P


LN_EPS = 1e-5
ROPE_BASE = 10000.0
F32 = jnp.float32
BF16 = jnp.bfloat16

CORE_GROUPS = [[0, 2, 4, 6], [1, 3, 5, 7]]
SIBLING = [(i, i ^ 1) for i in range(8)]


def mm(form, left, right):
    return jnp.einsum(form, left, right, preferred_element_type=F32)


def norm_stats(tensor):
    centered = tensor - jnp.mean(tensor, axis=-1, keepdims=True)
    inv_std = lax.rsqrt(jnp.mean(centered * centered, axis=-1, keepdims=True) + LN_EPS)
    return centered * inv_std, inv_std


def norm_backward(grad_hat, x_hat, inv_std):
    mean_grad = jnp.mean(grad_hat, axis=-1, keepdims=True)
    mean_proj = jnp.mean(grad_hat * x_hat, axis=-1, keepdims=True)
    return inv_std * (grad_hat - mean_grad - x_hat * mean_proj)


def attention_kernel(heads, kv_heads, head_dim, qkv_ref, ga_ref, cos_ref, sin_ref, norm_ref, out_ref, gqkv_ref, gnorm_ref):
    seq_len = qkv_ref.shape[0]
    group = heads // kv_heads
    scale = head_dim ** -0.5
    cosine, sine = cos_ref[...], sin_ref[...]
    even = lax.rem(lax.broadcasted_iota(jnp.int32, (seq_len, head_dim), 1), 2) == 0
    causal = (lax.broadcasted_iota(jnp.int32, (seq_len, seq_len), 0)
              >= lax.broadcasted_iota(jnp.int32, (seq_len, seq_len), 1))

    def turn(tensor, signed_sine):
        swapped = jnp.where(even, pltpu.roll(tensor, head_dim - 1, 1), pltpu.roll(tensor, 1, 1))
        return tensor * cosine + swapped * signed_sine

    def dot(left, right, left_dim, right_dim):
        return lax.dot_general(left, right, (((left_dim,), (right_dim,)), ((), ())), preferred_element_type=F32)

    def columns(index):
        return pl.ds(index * head_dim, head_dim)

    @pl.when(pl.program_id(0) == 0)
    def _():
        gnorm_ref[...] = jnp.zeros_like(gnorm_ref)

    def finish(index, grad_rot, hat, inv, gain):
        scaled = turn(grad_rot, -sine)
        gnorm_ref[pl.ds(index, 1), :] += jnp.sum(scaled * hat, axis=0, keepdims=True)
        gqkv_ref[:, columns(index)] = norm_backward(scaled * gain, hat, inv).astype(BF16)

    for kv in range(kv_heads):
        k_index, v_index = heads + kv, heads + kv_heads + kv
        k_hat, k_inv = norm_stats(qkv_ref[:, columns(k_index)].astype(F32))
        k_gain = norm_ref[pl.ds(k_index, 1), :]
        k_rot = turn(k_hat * k_gain, sine).astype(BF16)
        value = qkv_ref[:, columns(v_index)]
        grad_k = jnp.zeros((seq_len, head_dim), F32)
        grad_v = jnp.zeros((seq_len, head_dim), F32)
        for head in range(kv * group, (kv + 1) * group):
            q_hat, q_inv = norm_stats(qkv_ref[:, columns(head)].astype(F32))
            q_gain = norm_ref[pl.ds(head, 1), :]
            q_rot = turn(q_hat * q_gain, sine).astype(BF16)
            scores = jnp.where(causal, dot(q_rot, k_rot, 1, 1) * scale, -1e30)
            weights = jnp.exp(scores - jnp.max(scores, axis=-1, keepdims=True))
            probs = weights / jnp.sum(weights, axis=-1, keepdims=True)
            probs_bf = probs.astype(BF16)
            out_ref[:, columns(head)] = dot(probs_bf, value, 1, 0).astype(BF16)
            grad_out = ga_ref[:, columns(head)]
            grad_probs = dot(grad_out, value, 1, 1)
            grad_v += dot(probs_bf, grad_out, 0, 0)
            centre = jnp.sum(grad_probs * probs, axis=-1, keepdims=True)
            grad_scores = (probs * (grad_probs - centre) * scale).astype(BF16)
            grad_k += dot(grad_scores, q_rot, 0, 0)
            finish(head, dot(grad_scores, k_rot, 1, 0), q_hat, q_inv, q_gain)
        finish(k_index, grad_k, k_hat, k_inv, k_gain)
        gqkv_ref[:, columns(v_index)] = grad_v.astype(BF16)


def attention(qkv, grad_attn, cosine, sine, norm_full, batch, seq_len, heads, kv_heads, head_dim):
    tokens, width = qkv.shape

    def rows(columns):
        return pl.BlockSpec((seq_len, columns), lambda b: (b, 0))

    whole = pl.BlockSpec(norm_full.shape, lambda b: (0, 0))
    return pl.pallas_call(
        functools.partial(attention_kernel, heads, kv_heads, head_dim),
        grid=(batch,),
        in_specs=[rows(width), rows(heads * head_dim), rows(head_dim), rows(head_dim), whole],
        out_specs=[rows(heads * head_dim), rows(width), whole],
        out_shape=[jax.ShapeDtypeStruct((tokens, heads * head_dim), BF16),
                   jax.ShapeDtypeStruct((tokens, width), BF16),
                   jax.ShapeDtypeStruct(norm_full.shape, F32)],
        compiler_params=pltpu.CompilerParams(dimension_semantics=("arbitrary",), vmem_limit_bytes=32 * 1024 * 1024),
        cost_estimate=pl.CostEstimate(flops=12 * batch * heads * seq_len * seq_len * head_dim, bytes_accessed=10 * tokens * width,
                                      transcendentals=batch * heads * seq_len * seq_len),
        name="attention",
    )(qkv, grad_attn, cosine, sine, norm_full)


def split_model_dim(tensor, core, width):
    pieces = [lax.slice_in_dim(tensor, j * width, (j + 1) * width, axis=tensor.ndim - 1) for j in range(8)]
    even = jnp.concatenate(pieces[0::2], axis=-1)
    odd = jnp.concatenate(pieces[1::2], axis=-1)
    first = core == 0
    return jnp.where(first, even, odd), jnp.where(first, odd, even)


def join_model_dim(mine, other, core, width):
    first = core == 0
    even = jnp.where(first, mine, other)
    odd = jnp.where(first, other, mine)
    pieces = []
    for j in range(4):
        pieces += [even[..., j * width:(j + 1) * width], odd[..., j * width:(j + 1) * width]]
    return jnp.concatenate(pieces, axis=-1)


def gather_mine(shard):
    return lax.all_gather(shard, 'fsdp', axis=0, tiled=True, axis_index_groups=CORE_GROUPS)


def with_sibling(mine):
    return mine, lax.ppermute(mine, 'fsdp', SIBLING)


def after(value, event):
    return lax.optimization_barrier((value, event))[0]


def chain_sum(parts, rank, n):
    def chunk(part, offset):
        return lax.dynamic_index_in_dim(part, rank[offset % n], 0, keepdims=False)

    halves = range(len(parts))
    from_left = [None for _ in halves]
    from_right = [None for _ in halves]
    sent = []
    for step in range(n - 1):
        right = [(i, i + 1) for i in range(step + 1)]
        left = [(n - 1 - i, n - 2 - i) for i in range(step + 1)]
        if step:
            from_left, from_right = after((from_left, from_right), sent[-len(parts):])
            from_left, from_right = list(from_left), list(from_right)
        for h in halves:
            go_right, go_left = chunk(parts[h], n - 1 - step), chunk(parts[h], step + 1)
            if step:
                go_right = (go_right.astype(F32) + from_left[h].astype(F32)).astype(BF16)
                go_left = (go_left.astype(F32) + from_right[h].astype(F32)).astype(BF16)
            sent.append((go_right, go_left))
            from_left[h] = lax.ppermute(go_right, 'tp', right)
            from_right[h] = lax.ppermute(go_left, 'tp', left)
    total = [chunk(parts[h], 0).astype(F32) + from_left[h].astype(F32) + from_right[h].astype(F32) for h in halves]
    return total, [sent[k * len(parts):(k + 1) * len(parts)] for k in range(n - 1)]


def chain_gather(block, rank, n):
    zero = jnp.uint32(0)
    from_left, from_right = [], []
    go_right = go_left = block
    for step in range(n - 1):
        go_right = lax.ppermute(go_right, 'tp', [(i, i + 1) for i in range(step, n - 1)])
        go_left = lax.ppermute(go_left, 'tp', [(i, i - 1) for i in range(n - 1 - step, 0, -1)])
        from_left.append(go_right)
        from_right.append(go_left)
    whole = jnp.zeros((n,) + block.shape, block.dtype)
    own = after(block, (from_left[0], from_right[0]))
    whole = lax.dynamic_update_slice(whole, own[None], (rank[0], zero, zero))
    for k in range(1, n):
        piece = jnp.where(rank[0] >= k, from_left[k - 1], from_right[n - k - 1])
        whole = lax.dynamic_update_slice(whole, piece[None], (rank[n - k], zero, zero))
    return whole


def solution(mesh):
    act_spec = P('fsdp', None, None)
    col_spec = P('fsdp', 'tp')
    row_spec = P('tp', 'fsdp')
    weight_specs = (P('fsdp'), col_spec, col_spec, col_spec, row_spec, col_spec, col_spec, row_spec, row_spec, row_spec)
    in_specs = (act_spec, P('fsdp', None), act_spec) + weight_specs
    out_specs = (act_spec, act_spec) + weight_specs
    n_tp = mesh.shape['tp']
    n_fsdp = mesh.shape['fsdp']

    def device_step(hidden, positions, grad_layer, ln_weight, w_query, w_key, w_value, w_out, w_gate, w_up, w_down, q_norm, k_norm):
        batch, seq_len, model_dim = hidden.shape
        tokens = batch * seq_len
        width = ln_weight.shape[0]
        heads, kv_heads = q_norm.shape[0], k_norm.shape[0]
        dims_part = q_norm.shape[1]
        head_dim = dims_part * n_fsdp
        q_width, kv_width = heads * head_dim, kv_heads * head_dim
        qkv_width = q_width + 2 * kv_width
        fsdp = lax.axis_index('fsdp')
        core = lax.rem(fsdp, 2)
        tp = [lax.rem(lax.axis_index('tp') + k, n_tp).astype(jnp.uint32) for k in range(n_tp)]

        attn_shard = jnp.concatenate([w_query, w_key, w_value, w_out.T], axis=1)
        attn_mine = gather_mine(attn_shard)
        gate_mine = gather_mine(w_gate)
        up_mine = gather_mine(w_up)
        down_mine = gather_mine(w_down.T)
        attn_w = with_sibling(attn_mine)

        small = jnp.concatenate([ln_weight, q_norm.reshape(-1), k_norm.reshape(-1)])
        small_all = lax.all_gather(small, 'fsdp', axis=0, tiled=False).astype(F32)
        ln_full = small_all[:, :width].reshape(-1)
        q_part = heads * dims_part
        qn_full = small_all[:, width:width + q_part].reshape(n_fsdp, heads, dims_part).transpose(1, 0, 2).reshape(heads, head_dim)
        kn_full = small_all[:, width + q_part:].reshape(n_fsdp, kv_heads, dims_part).transpose(1, 0, 2).reshape(kv_heads, head_dim)
        norm_full = jnp.concatenate([qn_full, kn_full], axis=0)

        x_hat, _ = norm_stats(hidden.astype(F32))
        normed = (x_hat * ln_full).astype(BF16).reshape(tokens, model_dim)
        h_m, h_o = split_model_dim(normed, core, width)
        g_m, g_o = split_model_dim(grad_layer.reshape(tokens, model_dim), core, width)

        def contract(left, right):
            return mm('td,de->te', left[0], right[0]) + mm('td,de->te', left[1], right[1])

        def expand(left, right):
            return [mm('te,de->td', left, part) for part in right]

        def weight_grad(rows, cols):
            other = mm('td,te->de', rows[1], cols).astype(BF16)
            arrived = lax.ppermute(other, 'fsdp', SIBLING)
            total = (mm('td,te->de', rows[0], cols) + arrived.astype(F32)).astype(BF16)
            return lax.psum_scatter(total, 'fsdp', scatter_dimension=0, tiled=True, axis_index_groups=CORE_GROUPS)

        h_pair, g_pair = (h_m, h_o), (g_m, g_o)
        qkv_w = tuple(part[:, :qkv_width] for part in attn_w)
        out_w = tuple(part[:, qkv_width:] for part in attn_w)

        qkv = contract(h_pair, qkv_w).astype(BF16)
        grad_attn = contract(g_pair, out_w).astype(BF16)
        lane = lax.broadcasted_iota(jnp.int32, (1, head_dim), 1)
        inv_freq = ROPE_BASE ** (-((lane // 2) * 2).astype(F32) / head_dim)
        angles = positions.reshape(tokens, 1).astype(F32) * inv_freq
        cosine = jnp.cos(angles)
        sine = jnp.where(lane % 2 == 0, -1.0, 1.0) * jnp.sin(angles)
        attn_out, grad_qkv, norm_part = attention(qkv, grad_attn, cosine, sine, norm_full, batch, seq_len, heads, kv_heads, head_dim)
        attn_part = expand(attn_out, out_w)
        attn_dh = expand(grad_qkv, qkv_w)


        gate_w = with_sibling(after(gate_mine, attn_part))
        gate = contract(h_pair, gate_w).astype(BF16)
        up_w = with_sibling(after(up_mine, gate))
        up_proj = contract(h_pair, up_w).astype(BF16)
        down_w = with_sibling(after(down_mine, up_proj))
        gate_f32, up_f32 = gate.astype(F32), up_proj.astype(F32)
        sigma = jax.nn.sigmoid(gate_f32)
        gated_act = (gate_f32 * sigma * up_f32).astype(BF16)
        mlp_part = expand(gated_act, down_w)
        forward_part = [(a + b).astype(BF16) for a, b in zip(attn_part, mlp_part)]

        def own_chunk(tensor):
            return lax.dynamic_index_in_dim(tensor.reshape(n_tp, tokens // n_tp, model_dim), tp[0], 0, keepdims=False).astype(F32)

        def chunks(parts):
            return [part.reshape(n_tp, tokens // n_tp, part.shape[-1]) for part in parts]

        fwd_sum, fwd_sent = chain_sum(chunks(forward_part), tp, n_tp)
        hidden_chunk = own_chunk(hidden)
        out_chunk = (hidden_chunk + join_model_dim(fwd_sum[0], fwd_sum[1], core, width)).astype(BF16)
        layer_out = chain_gather(out_chunk, tp, n_tp)

        grad_act = contract((after(g_m, forward_part[0]), after(g_o, forward_part[1])), down_w)
        grad_gate = (grad_act * up_f32 * sigma * (1.0 + gate_f32 * (1.0 - sigma))).astype(BF16)
        grad_up = (grad_act * gate_f32 * sigma).astype(BF16)
        early_gate, early_up = after(grad_gate, fwd_sent[1]), after(grad_up, fwd_sent[2])
        dh_part = [(a + b + c).astype(BF16)
                   for a, b, c in zip(attn_dh, expand(early_gate, gate_w), expand(early_up, up_w))]
        dh_sum, _ = chain_sum(chunks(dh_part), tp, n_tp)

        grad_wqkv = weight_grad(h_pair, after(grad_qkv, forward_part))
        grad_wout = weight_grad(g_pair, after(attn_out, forward_part))
        grad_wdown = weight_grad(g_pair, after(gated_act, dh_part))
        grad_wgate = weight_grad(h_pair, after(grad_gate, dh_part))
        grad_wup = weight_grad(h_pair, after(grad_up, dh_part))
        grad_wqkv, grad_wout = after((grad_wqkv, grad_wout), dh_part)

        dh_sum = after(dh_sum, out_chunk)
        grad_normed = join_model_dim(dh_sum[0], dh_sum[1], core, width).astype(BF16).astype(F32)
        late_hidden, late_grad = after((own_chunk(hidden), own_chunk(grad_layer)), (out_chunk, dh_part))
        xc_hat, xc_inv = norm_stats(late_hidden)
        grad_chunk = (late_grad + norm_backward(grad_normed * ln_full, xc_hat, xc_inv)).astype(BF16)
        grad_hidden = chain_gather(grad_chunk, tp, n_tp)

        ln_part = jnp.sum(grad_normed * xc_hat, axis=0).reshape(n_fsdp, width)
        all_heads = heads + kv_heads
        head_part = norm_part.reshape(all_heads, n_fsdp, dims_part).transpose(1, 0, 2).reshape(n_fsdp, all_heads * dims_part)
        small_parts = lax.all_gather(jnp.concatenate([ln_part, head_part], axis=1), ('fsdp', 'tp'), axis=0, tiled=False)
        small_own = lax.dynamic_index_in_dim(small_parts, fsdp, 1, keepdims=False)
        grad_ln = jnp.sum(small_own[:, :width], axis=0)
        head_own = small_own[:, width:].reshape(n_fsdp, n_tp, all_heads * dims_part)
        head_own = jnp.sum(lax.dynamic_index_in_dim(head_own, tp[0], 1, keepdims=False), axis=0)
        norm_own = head_own.reshape(all_heads, dims_part)

        return (layer_out.reshape(hidden.shape), grad_hidden.reshape(hidden.shape), grad_ln, grad_wqkv[:, :q_width], grad_wqkv[:, q_width:q_width + kv_width],
                grad_wqkv[:, q_width + kv_width:], grad_wout.T, grad_wgate, grad_wup, grad_wdown.T,
                norm_own[:heads], norm_own[heads:])

    return jax.shard_map(device_step, mesh=mesh, in_specs=in_specs, out_specs=out_specs, check_vma=False)
```

```python
import functools

import jax
import jax.numpy as jnp
from jax import lax
from jax.experimental import pallas as pl
from jax.experimental.pallas import tpu as pltpu
from jax.sharding import PartitionSpec as P


LN_EPS = 1e-5
ROPE_BASE = 10000.0
F32 = jnp.float32
BF16 = jnp.bfloat16

CORE_GROUPS = [[0, 2, 4, 6], [1, 3, 5, 7]]
SIBLING = [(i, i ^ 1) for i in range(8)]


def mm(form, left, right):
    return jnp.einsum(form, left, right, preferred_element_type=F32)


def norm_stats(tensor):
    centered = tensor - jnp.mean(tensor, axis=-1, keepdims=True)
    inv_std = lax.rsqrt(jnp.mean(centered * centered, axis=-1, keepdims=True) + LN_EPS)
    return centered * inv_std, inv_std


def norm_backward(grad_hat, x_hat, inv_std):
    mean_grad = jnp.mean(grad_hat, axis=-1, keepdims=True)
    mean_proj = jnp.mean(grad_hat * x_hat, axis=-1, keepdims=True)
    return inv_std * (grad_hat - mean_grad - x_hat * mean_proj)


def attention_kernel(heads, kv_heads, head_dim, qkv_ref, ga_ref, cos_ref, sin_ref, norm_ref, out_ref, gqkv_ref, gnorm_ref):
    seq_len = qkv_ref.shape[0]
    group = heads // kv_heads
    scale = head_dim ** -0.5
    cosine, sine = cos_ref[...], sin_ref[...]
    even = lax.rem(lax.broadcasted_iota(jnp.int32, (seq_len, head_dim), 1), 2) == 0
    causal = (lax.broadcasted_iota(jnp.int32, (seq_len, seq_len), 0)
              >= lax.broadcasted_iota(jnp.int32, (seq_len, seq_len), 1))

    def turn(tensor, signed_sine):
        swapped = jnp.where(even, pltpu.roll(tensor, head_dim - 1, 1), pltpu.roll(tensor, 1, 1))
        return tensor * cosine + swapped * signed_sine

    def dot(left, right, left_dim, right_dim):
        return lax.dot_general(left, right, (((left_dim,), (right_dim,)), ((), ())), preferred_element_type=F32)

    def columns(index):
        return pl.ds(index * head_dim, head_dim)

    @pl.when(pl.program_id(0) == 0)
    def _():
        gnorm_ref[...] = jnp.zeros_like(gnorm_ref)

    def finish(index, grad_rot, hat, inv, gain):
        scaled = turn(grad_rot, -sine)
        gnorm_ref[pl.ds(index, 1), :] += jnp.sum(scaled * hat, axis=0, keepdims=True)
        gqkv_ref[:, columns(index)] = norm_backward(scaled * gain, hat, inv).astype(BF16)

    for kv in range(kv_heads):
        k_index, v_index = heads + kv, heads + kv_heads + kv
        k_hat, k_inv = norm_stats(qkv_ref[:, columns(k_index)].astype(F32))
        k_gain = norm_ref[pl.ds(k_index, 1), :]
        k_rot = turn(k_hat * k_gain, sine).astype(BF16)
        value = qkv_ref[:, columns(v_index)]
        grad_k = jnp.zeros((seq_len, head_dim), F32)
        grad_v = jnp.zeros((seq_len, head_dim), F32)
        for head in range(kv * group, (kv + 1) * group):
            q_hat, q_inv = norm_stats(qkv_ref[:, columns(head)].astype(F32))
            q_gain = norm_ref[pl.ds(head, 1), :]
            q_rot = turn(q_hat * q_gain, sine).astype(BF16)
            scores = jnp.where(causal, dot(q_rot, k_rot, 1, 1) * scale, -1e30)
            weights = jnp.exp(scores - jnp.max(scores, axis=-1, keepdims=True))
            probs = weights / jnp.sum(weights, axis=-1, keepdims=True)
            probs_bf = probs.astype(BF16)
            out_ref[:, columns(head)] = dot(probs_bf, value, 1, 0).astype(BF16)
            grad_out = ga_ref[:, columns(head)]
            grad_probs = dot(grad_out, value, 1, 1)
            grad_v += dot(probs_bf, grad_out, 0, 0)
            centre = jnp.sum(grad_probs * probs, axis=-1, keepdims=True)
            grad_scores = (probs * (grad_probs - centre) * scale).astype(BF16)
            grad_k += dot(grad_scores, q_rot, 0, 0)
            finish(head, dot(grad_scores, k_rot, 1, 0), q_hat, q_inv, q_gain)
        finish(k_index, grad_k, k_hat, k_inv, k_gain)
        gqkv_ref[:, columns(v_index)] = grad_v.astype(BF16)


def attention(qkv, grad_attn, cosine, sine, norm_full, batch, seq_len, heads, kv_heads, head_dim):
    tokens, width = qkv.shape

    def rows(columns):
        return pl.BlockSpec((seq_len, columns), lambda b: (b, 0))

    whole = pl.BlockSpec(norm_full.shape, lambda b: (0, 0))
    return pl.pallas_call(
        functools.partial(attention_kernel, heads, kv_heads, head_dim),
        grid=(batch,),
        in_specs=[rows(width), rows(heads * head_dim), rows(head_dim), rows(head_dim), whole],
        out_specs=[rows(heads * head_dim), rows(width), whole],
        out_shape=[jax.ShapeDtypeStruct((tokens, heads * head_dim), BF16),
                   jax.ShapeDtypeStruct((tokens, width), BF16),
                   jax.ShapeDtypeStruct(norm_full.shape, F32)],
        compiler_params=pltpu.CompilerParams(dimension_semantics=("arbitrary",), vmem_limit_bytes=32 * 1024 * 1024),
        cost_estimate=pl.CostEstimate(flops=12 * batch * heads * seq_len * seq_len * head_dim, bytes_accessed=10 * tokens * width,
                                      transcendentals=batch * heads * seq_len * seq_len),
        name="attention",
    )(qkv, grad_attn, cosine, sine, norm_full)


def split_model_dim(tensor, core, width):
    pieces = [lax.slice_in_dim(tensor, j * width, (j + 1) * width, axis=tensor.ndim - 1) for j in range(8)]
    even = jnp.concatenate(pieces[0::2], axis=-1)
    odd = jnp.concatenate(pieces[1::2], axis=-1)
    first = core == 0
    return jnp.where(first, even, odd), jnp.where(first, odd, even)


def join_model_dim(mine, other, core, width):
    first = core == 0
    even = jnp.where(first, mine, other)
    odd = jnp.where(first, other, mine)
    pieces = []
    for j in range(4):
        pieces += [even[..., j * width:(j + 1) * width], odd[..., j * width:(j + 1) * width]]
    return jnp.concatenate(pieces, axis=-1)


def gather_mine(shard):
    return lax.all_gather(shard, 'fsdp', axis=0, tiled=True, axis_index_groups=CORE_GROUPS)


def neighbours(bit):
    return [(i, i ^ bit) for i in range(8)]


def place(pieces, slots):
    zero = jnp.uint32(0)
    whole = jnp.zeros((len(pieces),) + pieces[0].shape, pieces[0].dtype)
    for piece, slot in zip(pieces, slots):
        whole = lax.dynamic_update_slice(whole, piece[None], (slot, zero, zero))
    return whole.reshape((-1,) + pieces[0].shape[1:])


def with_sibling(mine):
    return mine, lax.ppermute(mine, 'fsdp', SIBLING)


def after(value, event):
    return lax.optimization_barrier((value, event))[0]


def chain_sum(parts, rank, n):
    def chunk(part, offset):
        return lax.dynamic_index_in_dim(part, rank[offset % n], 0, keepdims=False)

    halves = range(len(parts))
    from_left = [None for _ in halves]
    from_right = [None for _ in halves]
    sent = []
    for step in range(n - 1):
        right = [(i, i + 1) for i in range(step + 1)]
        left = [(n - 1 - i, n - 2 - i) for i in range(step + 1)]
        if step:
            from_left, from_right = after((from_left, from_right), sent[-len(parts):])
            from_left, from_right = list(from_left), list(from_right)
        for h in halves:
            go_right, go_left = chunk(parts[h], n - 1 - step), chunk(parts[h], step + 1)
            if step:
                go_right = (go_right.astype(F32) + from_left[h].astype(F32)).astype(BF16)
                go_left = (go_left.astype(F32) + from_right[h].astype(F32)).astype(BF16)
            sent.append((go_right, go_left))
            from_left[h] = lax.ppermute(go_right, 'tp', right)
            from_right[h] = lax.ppermute(go_left, 'tp', left)
    total = [chunk(parts[h], 0).astype(F32) + from_left[h].astype(F32) + from_right[h].astype(F32) for h in halves]
    return total, [sent[k * len(parts):(k + 1) * len(parts)] for k in range(n - 1)]


def chain_gather(block, rank, n):
    zero = jnp.uint32(0)
    from_left, from_right = [], []
    go_right = go_left = block
    for step in range(n - 1):
        go_right = lax.ppermute(go_right, 'tp', [(i, i + 1) for i in range(step, n - 1)])
        go_left = lax.ppermute(go_left, 'tp', [(i, i - 1) for i in range(n - 1 - step, 0, -1)])
        from_left.append(go_right)
        from_right.append(go_left)
    whole = jnp.zeros((n,) + block.shape, block.dtype)
    own = after(block, (from_left[0], from_right[0]))
    whole = lax.dynamic_update_slice(whole, own[None], (rank[0], zero, zero))
    for k in range(1, n):
        piece = jnp.where(rank[0] >= k, from_left[k - 1], from_right[n - k - 1])
        whole = lax.dynamic_update_slice(whole, piece[None], (rank[n - k], zero, zero))
    return whole


def solution(mesh):
    act_spec = P('fsdp', None, None)
    col_spec = P('fsdp', 'tp')
    row_spec = P('tp', 'fsdp')
    weight_specs = (P('fsdp'), col_spec, col_spec, col_spec, row_spec, col_spec, col_spec, row_spec, row_spec, row_spec)
    in_specs = (act_spec, P('fsdp', None), act_spec) + weight_specs
    out_specs = (act_spec, act_spec) + weight_specs
    n_tp = mesh.shape['tp']
    n_fsdp = mesh.shape['fsdp']

    def device_step(hidden, positions, grad_layer, ln_weight, w_query, w_key, w_value, w_out, w_gate, w_up, w_down, q_norm, k_norm):
        batch, seq_len, model_dim = hidden.shape
        tokens = batch * seq_len
        width = ln_weight.shape[0]
        heads, kv_heads = q_norm.shape[0], k_norm.shape[0]
        dims_part = q_norm.shape[1]
        head_dim = dims_part * n_fsdp
        q_width, kv_width = heads * head_dim, kv_heads * head_dim
        qkv_width = q_width + 2 * kv_width
        fsdp = lax.axis_index('fsdp')
        core = lax.rem(fsdp, 2)
        tp = [lax.rem(lax.axis_index('tp') + k, n_tp).astype(jnp.uint32) for k in range(n_tp)]

        attn_shard = jnp.concatenate([w_query, w_key, w_value, w_out.T], axis=1)
        attn_mine = gather_mine(attn_shard)
        gate_mine = gather_mine(w_gate)
        up_y, up_x = lax.ppermute(w_up, 'fsdp', neighbours(4)), lax.ppermute(w_up, 'fsdp', neighbours(2))
        up_far = lax.ppermute(up_y, 'fsdp', neighbours(2))
        down_shard = after(w_down.T, up_y)
        down_y, down_x = lax.ppermute(down_shard, 'fsdp', neighbours(4)), lax.ppermute(down_shard, 'fsdp', neighbours(2))
        down_far = lax.ppermute(down_y, 'fsdp', neighbours(2))
        chip = (fsdp // 2).astype(jnp.uint32)
        slots = [chip ^ jnp.uint32(k) for k in range(4)]

        small = jnp.concatenate([ln_weight, q_norm.reshape(-1), k_norm.reshape(-1)])
        small_all = lax.all_gather(small, 'fsdp', axis=0, tiled=False).astype(F32)
        ln_full = small_all[:, :width].reshape(-1)
        q_part = heads * dims_part
        qn_full = small_all[:, width:width + q_part].reshape(n_fsdp, heads, dims_part).transpose(1, 0, 2).reshape(heads, head_dim)
        kn_full = small_all[:, width + q_part:].reshape(n_fsdp, kv_heads, dims_part).transpose(1, 0, 2).reshape(kv_heads, head_dim)
        norm_full = jnp.concatenate([qn_full, kn_full], axis=0)

        x_hat, _ = norm_stats(hidden.astype(F32))
        normed = (x_hat * ln_full).astype(BF16).reshape(tokens, model_dim)
        h_m, h_o = split_model_dim(normed, core, width)
        g_m, g_o = split_model_dim(grad_layer.reshape(tokens, model_dim), core, width)

        def contract(left, right):
            return mm('td,de->te', left[0], right[0]) + mm('td,de->te', left[1], right[1])

        def expand(left, right):
            return [mm('te,de->td', left, part) for part in right]

        def weight_grad(rows, cols):
            other = mm('td,te->de', rows[1], cols).astype(BF16)
            arrived = lax.ppermute(other, 'fsdp', SIBLING)
            total = (mm('td,te->de', rows[0], cols) + arrived.astype(F32)).astype(BF16)
            return lax.psum_scatter(total, 'fsdp', scatter_dimension=0, tiled=True, axis_index_groups=CORE_GROUPS)

        h_pair, g_pair = (h_m, h_o), (g_m, g_o)
        lane = lax.broadcasted_iota(jnp.int32, (1, head_dim), 1)
        inv_freq = ROPE_BASE ** (-((lane // 2) * 2).astype(F32) / head_dim)
        angles = positions.reshape(tokens, 1).astype(F32) * inv_freq
        cosine = jnp.cos(angles)
        sine = jnp.where(lane % 2 == 0, -1.0, 1.0) * jnp.sin(angles)
        attn_w = with_sibling(after(attn_mine, (h_pair, g_pair, cosine, up_y)))
        qkv_w = tuple(part[:, :qkv_width] for part in attn_w)
        out_w = tuple(part[:, qkv_width:] for part in attn_w)

        qkv = contract((after(h_m, up_y), h_o), qkv_w).astype(BF16)
        grad_attn = contract(g_pair, out_w).astype(BF16)
        attn_out, grad_qkv, norm_part = attention(qkv, grad_attn, cosine, sine, norm_full, batch, seq_len, heads, kv_heads, head_dim)
        attn_part = expand(after(attn_out, down_y), out_w)
        attn_dh = expand(grad_qkv, qkv_w)


        up_w = with_sibling(place(after((w_up, up_x, up_y, up_far), attn_out), slots))
        up_proj = contract((after(h_m, attn_part), h_o), up_w).astype(BF16)
        gate_w = with_sibling(after(gate_mine, up_proj))
        gate = contract(h_pair, gate_w).astype(BF16)
        down_w = with_sibling(place(after((down_shard, down_x, down_y, down_far), gate), slots))
        gate_f32, up_f32 = gate.astype(F32), up_proj.astype(F32)
        sigma = jax.nn.sigmoid(gate_f32)
        gated_act = (gate_f32 * sigma * up_f32).astype(BF16)
        mlp_part = expand(gated_act, down_w)
        forward_part = [(a + b).astype(BF16) for a, b in zip(attn_part, mlp_part)]

        def own_chunk(tensor):
            return lax.dynamic_index_in_dim(tensor.reshape(n_tp, tokens // n_tp, model_dim), tp[0], 0, keepdims=False).astype(F32)

        def chunks(parts):
            return [part.reshape(n_tp, tokens // n_tp, part.shape[-1]) for part in parts]

        fwd_sum, fwd_sent = chain_sum(chunks(forward_part), tp, n_tp)
        hidden_chunk = own_chunk(hidden)
        out_chunk = (hidden_chunk + join_model_dim(fwd_sum[0], fwd_sum[1], core, width)).astype(BF16)
        layer_out = chain_gather(out_chunk, tp, n_tp)

        grad_act = contract((after(g_m, forward_part[0]), after(g_o, forward_part[1])), down_w)
        grad_gate = (grad_act * up_f32 * sigma * (1.0 + gate_f32 * (1.0 - sigma))).astype(BF16)
        grad_up = (grad_act * gate_f32 * sigma).astype(BF16)
        early_gate, early_up = after(grad_gate, fwd_sent[1]), after(grad_up, fwd_sent[2])
        dh_part = [(a + b + c).astype(BF16)
                   for a, b, c in zip(attn_dh, expand(early_gate, gate_w), expand(early_up, up_w))]
        dh_sum, _ = chain_sum(chunks(dh_part), tp, n_tp)

        grad_wqkv = weight_grad(h_pair, after(grad_qkv, forward_part))
        grad_wout = weight_grad(g_pair, after(attn_out, forward_part))
        grad_wdown = weight_grad(g_pair, after(gated_act, dh_part))
        grad_wgate = weight_grad(h_pair, after(grad_gate, dh_part))
        grad_wup = weight_grad(h_pair, after(grad_up, dh_part))
        grad_wqkv, grad_wout = after((grad_wqkv, grad_wout), dh_part)

        dh_sum = after(dh_sum, out_chunk)
        grad_normed = join_model_dim(dh_sum[0], dh_sum[1], core, width).astype(BF16).astype(F32)
        late_hidden, late_grad = after((own_chunk(hidden), own_chunk(grad_layer)), (out_chunk, dh_part))
        xc_hat, xc_inv = norm_stats(late_hidden)
        grad_chunk = (late_grad + norm_backward(grad_normed * ln_full, xc_hat, xc_inv)).astype(BF16)
        grad_hidden = chain_gather(grad_chunk, tp, n_tp)

        ln_part = jnp.sum(grad_normed * xc_hat, axis=0).reshape(n_fsdp, width)
        all_heads = heads + kv_heads
        head_part = norm_part.reshape(all_heads, n_fsdp, dims_part).transpose(1, 0, 2).reshape(n_fsdp, all_heads * dims_part)
        small_parts = lax.all_gather(jnp.concatenate([ln_part, head_part], axis=1), 'fsdp', axis=0, tiled=False)
        small_own = jnp.sum(lax.dynamic_index_in_dim(small_parts, fsdp, 1, keepdims=False), axis=0)
        norm_own = small_own[width:].reshape(all_heads, dims_part)
        grad_ln = jnp.sum(lax.all_gather(small_own[:width], 'tp', axis=0, tiled=False), axis=0)

        return (layer_out.reshape(hidden.shape), grad_hidden.reshape(hidden.shape), grad_ln, grad_wqkv[:, :q_width], grad_wqkv[:, q_width:q_width + kv_width],
                grad_wqkv[:, q_width + kv_width:], grad_wout.T, grad_wgate, grad_wup, grad_wdown.T,
                norm_own[:heads], norm_own[heads:])

    return jax.shard_map(device_step, mesh=mesh, in_specs=in_specs, out_specs=out_specs, check_vma=False)
```

```python
import functools

import jax
import jax.numpy as jnp
from jax import lax
from jax.experimental import pallas as pl
from jax.experimental.pallas import tpu as pltpu
from jax.sharding import PartitionSpec as P


LN_EPS = 1e-5
ROPE_BASE = 10000.0
F32 = jnp.float32
BF16 = jnp.bfloat16

CORE_GROUPS = [[0, 2, 4, 6], [1, 3, 5, 7]]
SIBLING = [(i, i ^ 1) for i in range(8)]


def mm(form, left, right):
    return jnp.einsum(form, left, right, preferred_element_type=F32)


def norm_stats(tensor):
    centered = tensor - jnp.mean(tensor, axis=-1, keepdims=True)
    inv_std = lax.rsqrt(jnp.mean(centered * centered, axis=-1, keepdims=True) + LN_EPS)
    return centered * inv_std, inv_std


def norm_backward(grad_hat, x_hat, inv_std):
    mean_grad = jnp.mean(grad_hat, axis=-1, keepdims=True)
    mean_proj = jnp.mean(grad_hat * x_hat, axis=-1, keepdims=True)
    return inv_std * (grad_hat - mean_grad - x_hat * mean_proj)


def attention_kernel(heads, kv_heads, head_dim, qkv_ref, ga_ref, cos_ref, sin_ref, norm_ref, out_ref, gqkv_ref, gnorm_ref):
    seq_len = qkv_ref.shape[0]
    group = heads // kv_heads
    scale = head_dim ** -0.5
    cosine, sine = cos_ref[...], sin_ref[...]
    even = lax.rem(lax.broadcasted_iota(jnp.int32, (seq_len, head_dim), 1), 2) == 0
    causal = (lax.broadcasted_iota(jnp.int32, (seq_len, seq_len), 0)
              >= lax.broadcasted_iota(jnp.int32, (seq_len, seq_len), 1))

    def turn(tensor, signed_sine):
        swapped = jnp.where(even, pltpu.roll(tensor, head_dim - 1, 1), pltpu.roll(tensor, 1, 1))
        return tensor * cosine + swapped * signed_sine

    def dot(left, right, left_dim, right_dim):
        return lax.dot_general(left, right, (((left_dim,), (right_dim,)), ((), ())), preferred_element_type=F32)

    def columns(index):
        return pl.ds(index * head_dim, head_dim)

    @pl.when(pl.program_id(0) == 0)
    def _():
        gnorm_ref[...] = jnp.zeros_like(gnorm_ref)

    def finish(index, grad_rot, hat, inv, gain):
        scaled = turn(grad_rot, -sine)
        gnorm_ref[pl.ds(index, 1), :] += jnp.sum(scaled * hat, axis=0, keepdims=True)
        gqkv_ref[:, columns(index)] = norm_backward(scaled * gain, hat, inv).astype(BF16)

    for kv in range(kv_heads):
        k_index, v_index = heads + kv, heads + kv_heads + kv
        k_hat, k_inv = norm_stats(qkv_ref[:, columns(k_index)].astype(F32))
        k_gain = norm_ref[pl.ds(k_index, 1), :]
        k_rot = turn(k_hat * k_gain, sine).astype(BF16)
        value = qkv_ref[:, columns(v_index)]
        grad_k = jnp.zeros((seq_len, head_dim), F32)
        grad_v = jnp.zeros((seq_len, head_dim), F32)
        for head in range(kv * group, (kv + 1) * group):
            q_hat, q_inv = norm_stats(qkv_ref[:, columns(head)].astype(F32))
            q_gain = norm_ref[pl.ds(head, 1), :]
            q_rot = turn(q_hat * q_gain, sine).astype(BF16)
            scores = jnp.where(causal, dot(q_rot, k_rot, 1, 1) * scale, -1e30)
            weights = jnp.exp(scores - jnp.max(scores, axis=-1, keepdims=True))
            probs = weights / jnp.sum(weights, axis=-1, keepdims=True)
            probs_bf = probs.astype(BF16)
            out_ref[:, columns(head)] = dot(probs_bf, value, 1, 0).astype(BF16)
            grad_out = ga_ref[:, columns(head)]
            grad_probs = dot(grad_out, value, 1, 1)
            grad_v += dot(probs_bf, grad_out, 0, 0)
            centre = jnp.sum(grad_probs * probs, axis=-1, keepdims=True)
            grad_scores = (probs * (grad_probs - centre) * scale).astype(BF16)
            grad_k += dot(grad_scores, q_rot, 0, 0)
            finish(head, dot(grad_scores, k_rot, 1, 0), q_hat, q_inv, q_gain)
        finish(k_index, grad_k, k_hat, k_inv, k_gain)
        gqkv_ref[:, columns(v_index)] = grad_v.astype(BF16)


def attention(qkv, grad_attn, cosine, sine, norm_full, batch, seq_len, heads, kv_heads, head_dim):
    tokens, width = qkv.shape

    def rows(columns):
        return pl.BlockSpec((seq_len, columns), lambda b: (b, 0))

    whole = pl.BlockSpec(norm_full.shape, lambda b: (0, 0))
    return pl.pallas_call(
        functools.partial(attention_kernel, heads, kv_heads, head_dim),
        grid=(batch,),
        in_specs=[rows(width), rows(heads * head_dim), rows(head_dim), rows(head_dim), whole],
        out_specs=[rows(heads * head_dim), rows(width), whole],
        out_shape=[jax.ShapeDtypeStruct((tokens, heads * head_dim), BF16),
                   jax.ShapeDtypeStruct((tokens, width), BF16),
                   jax.ShapeDtypeStruct(norm_full.shape, F32)],
        compiler_params=pltpu.CompilerParams(dimension_semantics=("arbitrary",), vmem_limit_bytes=32 * 1024 * 1024),
        cost_estimate=pl.CostEstimate(flops=12 * batch * heads * seq_len * seq_len * head_dim, bytes_accessed=10 * tokens * width,
                                      transcendentals=batch * heads * seq_len * seq_len),
        name="attention",
    )(qkv, grad_attn, cosine, sine, norm_full)


def split_model_dim(tensor, core, width):
    pieces = [lax.slice_in_dim(tensor, j * width, (j + 1) * width, axis=tensor.ndim - 1) for j in range(8)]
    even = jnp.concatenate(pieces[0::2], axis=-1)
    odd = jnp.concatenate(pieces[1::2], axis=-1)
    first = core == 0
    return jnp.where(first, even, odd), jnp.where(first, odd, even)


def join_model_dim(mine, other, core, width):
    first = core == 0
    even = jnp.where(first, mine, other)
    odd = jnp.where(first, other, mine)
    pieces = []
    for j in range(4):
        pieces += [even[..., j * width:(j + 1) * width], odd[..., j * width:(j + 1) * width]]
    return jnp.concatenate(pieces, axis=-1)


def gather_mine(shard):
    return lax.all_gather(shard, 'fsdp', axis=0, tiled=True, axis_index_groups=CORE_GROUPS)


def with_sibling(mine):
    return mine, lax.ppermute(mine, 'fsdp', SIBLING)


def after(value, event):
    return lax.optimization_barrier((value, event))[0]


def chain_sum(parts, rank, n):
    def chunk(part, offset):
        return lax.dynamic_index_in_dim(part, rank[offset % n], 0, keepdims=False)

    halves = range(len(parts))
    from_left = [None for _ in halves]
    from_right = [None for _ in halves]
    sent = []
    for step in range(n - 1):
        right = [(i, i + 1) for i in range(step + 1)]
        left = [(n - 1 - i, n - 2 - i) for i in range(step + 1)]
        if step:
            from_left, from_right = after((from_left, from_right), sent[-len(parts):])
            from_left, from_right = list(from_left), list(from_right)
        for h in halves:
            go_right, go_left = chunk(parts[h], n - 1 - step), chunk(parts[h], step + 1)
            if step:
                go_right = (go_right.astype(F32) + from_left[h].astype(F32)).astype(BF16)
                go_left = (go_left.astype(F32) + from_right[h].astype(F32)).astype(BF16)
            sent.append((go_right, go_left))
            from_left[h] = lax.ppermute(go_right, 'tp', right)
            from_right[h] = lax.ppermute(go_left, 'tp', left)
    total = [chunk(parts[h], 0).astype(F32) + from_left[h].astype(F32) + from_right[h].astype(F32) for h in halves]
    return total, [sent[k * len(parts):(k + 1) * len(parts)] for k in range(n - 1)]


def chain_gather(block, rank, n):
    zero = jnp.uint32(0)
    from_left, from_right = [], []
    go_right = go_left = block
    for step in range(n - 1):
        go_right = lax.ppermute(go_right, 'tp', [(i, i + 1) for i in range(step, n - 1)])
        go_left = lax.ppermute(go_left, 'tp', [(i, i - 1) for i in range(n - 1 - step, 0, -1)])
        from_left.append(go_right)
        from_right.append(go_left)
    whole = jnp.zeros((n,) + block.shape, block.dtype)
    own = after(block, (from_left[0], from_right[0]))
    whole = lax.dynamic_update_slice(whole, own[None], (rank[0], zero, zero))
    for k in range(1, n):
        piece = jnp.where(rank[0] >= k, from_left[k - 1], from_right[n - k - 1])
        whole = lax.dynamic_update_slice(whole, piece[None], (rank[n - k], zero, zero))
    return whole


def solution(mesh):
    act_spec = P('fsdp', None, None)
    col_spec = P('fsdp', 'tp')
    row_spec = P('tp', 'fsdp')
    weight_specs = (P('fsdp'), col_spec, col_spec, col_spec, row_spec, col_spec, col_spec, row_spec, row_spec, row_spec)
    in_specs = (act_spec, P('fsdp', None), act_spec) + weight_specs
    out_specs = (act_spec, act_spec) + weight_specs
    n_tp = mesh.shape['tp']
    n_fsdp = mesh.shape['fsdp']

    def device_step(hidden, positions, grad_layer, ln_weight, w_query, w_key, w_value, w_out, w_gate, w_up, w_down, q_norm, k_norm):
        batch, seq_len, model_dim = hidden.shape
        tokens = batch * seq_len
        width = ln_weight.shape[0]
        heads, kv_heads = q_norm.shape[0], k_norm.shape[0]
        dims_part = q_norm.shape[1]
        head_dim = dims_part * n_fsdp
        q_width, kv_width = heads * head_dim, kv_heads * head_dim
        qkv_width = q_width + 2 * kv_width
        fsdp = lax.axis_index('fsdp')
        core = lax.rem(fsdp, 2)
        tp = [lax.rem(lax.axis_index('tp') + k, n_tp).astype(jnp.uint32) for k in range(n_tp)]

        attn_shard = jnp.concatenate([w_query, w_key, w_value, w_out.T], axis=1)
        attn_mine = gather_mine(attn_shard)
        gate_mine = gather_mine(w_gate)
        up_mine = gather_mine(w_up)
        down_mine = gather_mine(w_down.T)
        attn_w = with_sibling(attn_mine)

        small = jnp.concatenate([ln_weight, q_norm.reshape(-1), k_norm.reshape(-1)])
        small_all = lax.all_gather(small, 'fsdp', axis=0, tiled=False).astype(F32)
        ln_full = small_all[:, :width].reshape(-1)
        q_part = heads * dims_part
        qn_full = small_all[:, width:width + q_part].reshape(n_fsdp, heads, dims_part).transpose(1, 0, 2).reshape(heads, head_dim)
        kn_full = small_all[:, width + q_part:].reshape(n_fsdp, kv_heads, dims_part).transpose(1, 0, 2).reshape(kv_heads, head_dim)
        norm_full = jnp.concatenate([qn_full, kn_full], axis=0)

        x_hat, _ = norm_stats(hidden.astype(F32))
        normed = (x_hat * ln_full).astype(BF16).reshape(tokens, model_dim)
        h_m, h_o = split_model_dim(normed, core, width)
        g_m, g_o = split_model_dim(grad_layer.reshape(tokens, model_dim), core, width)

        def contract(left, right):
            return mm('td,de->te', left[0], right[0]) + mm('td,de->te', left[1], right[1])

        def expand(left, right):
            return [mm('te,de->td', left, part) for part in right]

        def weight_total(rows, cols):
            other = mm('td,te->de', rows[1], cols).astype(BF16)
            arrived = lax.ppermute(other, 'fsdp', SIBLING)
            return (mm('td,te->de', rows[0], cols) + arrived.astype(F32)).astype(BF16)

        def scatter(total):
            return lax.psum_scatter(total, 'fsdp', scatter_dimension=0, tiled=True, axis_index_groups=CORE_GROUPS)

        h_pair, g_pair = (h_m, h_o), (g_m, g_o)
        qkv_w = tuple(part[:, :qkv_width] for part in attn_w)
        out_w = tuple(part[:, qkv_width:] for part in attn_w)

        qkv = contract(h_pair, qkv_w).astype(BF16)
        grad_attn = contract(g_pair, out_w).astype(BF16)
        lane = lax.broadcasted_iota(jnp.int32, (1, head_dim), 1)
        inv_freq = ROPE_BASE ** (-((lane // 2) * 2).astype(F32) / head_dim)
        angles = positions.reshape(tokens, 1).astype(F32) * inv_freq
        cosine = jnp.cos(angles)
        sine = jnp.where(lane % 2 == 0, -1.0, 1.0) * jnp.sin(angles)
        attn_out, grad_qkv, norm_part = attention(qkv, grad_attn, cosine, sine, norm_full, batch, seq_len, heads, kv_heads, head_dim)
        attn_part = expand(attn_out, out_w)
        attn_dh = expand(grad_qkv, qkv_w)


        out_total = weight_total(g_pair, after(attn_out, gate_mine))
        qkv_total = weight_total(h_pair, after(grad_qkv, gate_mine))
        gate_w = with_sibling(after(gate_mine, attn_part))
        gate = contract(h_pair, gate_w).astype(BF16)
        up_w = with_sibling(after(up_mine, (gate, out_total)))
        up_proj = contract(h_pair, up_w).astype(BF16)
        down_w = with_sibling(after(down_mine, (up_proj, qkv_total, attn_dh)))
        gate_f32, up_f32 = gate.astype(F32), up_proj.astype(F32)
        sigma = jax.nn.sigmoid(gate_f32)
        gated_act = (gate_f32 * sigma * up_f32).astype(BF16)
        mlp_part = expand(gated_act, down_w)
        forward_part = [(a + b).astype(BF16) for a, b in zip(attn_part, mlp_part)]

        def own_chunk(tensor):
            return lax.dynamic_index_in_dim(tensor.reshape(n_tp, tokens // n_tp, model_dim), tp[0], 0, keepdims=False).astype(F32)

        def chunks(parts):
            return [part.reshape(n_tp, tokens // n_tp, part.shape[-1]) for part in parts]

        fwd_sum, fwd_sent = chain_sum(chunks(forward_part), tp, n_tp)
        hidden_chunk = own_chunk(hidden)
        out_chunk = (hidden_chunk + join_model_dim(fwd_sum[0], fwd_sum[1], core, width)).astype(BF16)
        layer_out = chain_gather(out_chunk, tp, n_tp)

        grad_act = contract((after(g_m, forward_part[0]), after(g_o, forward_part[1])), down_w)
        grad_gate = (grad_act * up_f32 * sigma * (1.0 + gate_f32 * (1.0 - sigma))).astype(BF16)
        grad_up = (grad_act * gate_f32 * sigma).astype(BF16)
        early_gate, early_up = after(grad_gate, fwd_sent[1]), after(grad_up, fwd_sent[2])
        dh_early = [a + b for a, b in zip(attn_dh, expand(early_gate, gate_w))]
        dh_part = [(a + b).astype(BF16) for a, b in zip(dh_early, expand(early_up, up_w))]
        dh_sum, _ = chain_sum(chunks(dh_part), tp, n_tp)

        grad_wout, grad_wqkv = scatter(after(out_total, down_mine)), scatter(after(qkv_total, down_mine))
        grad_wdown = scatter(weight_total(g_pair, after(gated_act, dh_part)))
        grad_wgate = scatter(weight_total(h_pair, after(grad_gate, dh_part)))
        grad_wup = scatter(weight_total(h_pair, after(grad_up, dh_part)))
        grad_wqkv, grad_wout = after((grad_wqkv, grad_wout), dh_sum)

        dh_sum = after(dh_sum, out_chunk)
        grad_normed = join_model_dim(dh_sum[0], dh_sum[1], core, width).astype(BF16).astype(F32)
        late_hidden, late_grad = after((own_chunk(hidden), own_chunk(grad_layer)), (out_chunk, dh_part))
        xc_hat, xc_inv = norm_stats(late_hidden)
        grad_chunk = (late_grad + norm_backward(grad_normed * ln_full, xc_hat, xc_inv)).astype(BF16)
        grad_hidden = chain_gather(grad_chunk, tp, n_tp)

        ln_part = jnp.sum(grad_normed * xc_hat, axis=0).reshape(n_fsdp, width)
        all_heads = heads + kv_heads
        head_part = norm_part.reshape(all_heads, n_fsdp, dims_part).transpose(1, 0, 2).reshape(n_fsdp, all_heads * dims_part)
        small_block = jnp.concatenate([ln_part, head_part], axis=1)
        small_parts = lax.all_gather(small_block, 'fsdp', axis=0, tiled=False)
        small_own = jnp.sum(lax.dynamic_index_in_dim(small_parts, fsdp, 1, keepdims=False), axis=0)
        norm_own = small_own[width:].reshape(all_heads, dims_part)
        ln_own = small_own[:width]
        grad_ln = ln_own
        for shift in range(1, n_tp):
            grad_ln += lax.ppermute(ln_own, 'tp', [(i, (i + shift) % n_tp) for i in range(n_tp)])

        return (layer_out.reshape(hidden.shape), grad_hidden.reshape(hidden.shape), grad_ln, grad_wqkv[:, :q_width], grad_wqkv[:, q_width:q_width + kv_width],
                grad_wqkv[:, q_width + kv_width:], grad_wout.T, grad_wgate, grad_wup, grad_wdown.T,
                norm_own[:heads], norm_own[heads:])

    return jax.shard_map(device_step, mesh=mesh, in_specs=in_specs, out_specs=out_specs, check_vma=False)
```
